32 devices in a mesh: sub: 4 (over x, core), gx: 8 (over z, y).
Axes of the slice: x: 2, y: 2, z: 4, core: 2. Of those that a mesh axis runs over, the one named last changes fastest.
Arguments:
- value_field: float32 [8, 64, 256, 256], P('sub', 'gx'), may hold values from -6 to 6
- speed_field: float32 [8, 64, 256, 256], P('sub', 'gx'), may hold values from 0.25 to 2
- drift_matrix: float32 [8, 3, 3], P('sub'), may hold values from -0.5 to 0.5
- drift_offset: float32 [8, 3], P('sub'), may hold values from -0.5 to 0.5
- control_bound: float32 [8, 3], P('sub'), may hold values from 0.5 to 1
- partner_table: int32 [8], replicated, may hold values from 0 to 7, as said below
- dropped_dim: int32 [8], P('sub'), may hold values from 1 to 2, as said below
Outputs:
- final_value: float32 [8, 64, 256, 256], P('sub', 'gx')
- shared_plane: float32 [8, 64, 256], P('sub', 'gx')
The draws below stay inside these ranges and needn't reach their ends.
Inputs may be any that keep to these rules, and one draw needn't show every extreme that they name: `partner_table`: a permutation of the 8 subsystems that forms a single cycle through all of them, so no subsystem is its own partner. `dropped_dim`: half of the subsystems drop dimension 1 and half dimension 2.
All inputs are finite; a program needn't handle non-finite values.
Results may differ from the reference program's by a relative error of at most 0.00075.
Values sent between devices are 32-bit elements; how exact they have to be, the bound alone decides.
A program may use at most 128 MiB of HBM per device.

```python
import math
import jax
import jax.numpy as jnp
from jax import lax

N = 256
STEPS = 2
SUBS = 8
NX = 64


def draw_partner_table(key, part):
    order = jax.random.permutation(jax.random.fold_in(key, 11), SUBS).astype(jnp.int32)
    table = jnp.zeros((SUBS,), jnp.int32).at[order].set(jnp.roll(order, -1))
    return table.astype(jnp.int32)


def draw_dropped_dim(key, part):
    order = jax.random.permutation(jax.random.fold_in(key, 23), SUBS).astype(jnp.int32)
    return (1 + order % 2).astype(jnp.int32)


def steps_of(own_key, shape, pieces, least, high):
    loudness = 1.0
    for axis_at, blocks in pieces:
        draws = jax.random.uniform(jax.random.fold_in(jax.random.fold_in(own_key, 6), axis_at), (blocks,), jnp.float32, least / len(pieces), high / len(pieces))
        loudness = loudness * jnp.repeat(jnp.exp(draws), shape[axis_at] // blocks).reshape((-1,) + (1,) * (len(shape) - 1 - axis_at))
    return loudness


def gaussian(key, extent, scale, most, cuts=(), kind=jnp.bfloat16):
    loudness = steps_of(key, extent, cuts, -0.22, 0.18) if cuts else 1.0
    result = jax.random.normal(key, extent, jnp.float32) * scale * loudness
    return jnp.minimum(jnp.maximum(result, -most), most).astype(kind)


def setup_inputs(seed: int = 0) -> dict:
    key_list = jax.random.split(jax.random.key(seed), 8)
    value_field = gaussian(key_list[0], (SUBS, NX, N, N), 1.0, 6.0, ((0, 4), (1, 8)), jnp.float32)
    speed_field = jnp.clip(jnp.exp(math.log(2.0) - 2.0794415 * jax.random.uniform(key_list[1], (SUBS, NX, N, N), jnp.float32) ** steps_of(key_list[1], (SUBS, NX, N, N), ((0, 4), (1, 8)), -0.2, 0.2)), 0.25, 2.0)
    drift_matrix = jnp.clip(jax.random.uniform(key_list[2], (SUBS, 3, 3), jnp.float32, -0.5, 0.5) * steps_of(key_list[2], (SUBS, 3, 3), ((0, 4),), -0.4, 0.0), -0.5, 0.5)
    drift_offset = jnp.clip(jax.random.uniform(key_list[3], (SUBS, 3), jnp.float32, -0.5, 0.5) * steps_of(key_list[3], (SUBS, 3), ((0, 4),), -0.4, 0.0), -0.5, 0.5)
    control_bound = jnp.clip(0.5 + 0.5 * jax.random.uniform(key_list[4], (SUBS, 3), jnp.float32) ** steps_of(key_list[4], (SUBS, 3), ((0, 4),), -0.2, 0.2), 0.5, 1.0)
    partner_table = draw_partner_table(jax.random.fold_in(key_list[7], 71), 0)
    dropped_dim = draw_dropped_dim(jax.random.fold_in(key_list[7], 71), 0)
    return {"value_field": value_field, "speed_field": speed_field, "drift_matrix": drift_matrix, "drift_offset": drift_offset, "control_bound": control_bound, "partner_table": partner_table, "dropped_dim": dropped_dim}


def smaller(first, second):
    return jnp.where(jnp.abs(first) <= jnp.abs(second), first, second)


def one_sided(extended, dim_index, step_size):
    cell_count = extended.shape[dim_index] - 4

    def shifted(offset):
        return lax.slice_in_dim(extended, 2 + offset, 2 + offset + cell_count, axis=dim_index)

    back_two = shifted(-2)
    back_one = shifted(-1)
    middle = shifted(0)
    ahead_one = shifted(1)
    ahead_two = shifted(2)
    curve_back = back_two - 2.0 * back_one + middle
    curve_mid = back_one - 2.0 * middle + ahead_one
    curve_ahead = middle - 2.0 * ahead_one + ahead_two
    minus_side = (middle - back_one) / step_size + smaller(curve_back, curve_mid) / (2.0 * step_size)
    plus_side = (ahead_one - middle) / step_size - smaller(curve_mid, curve_ahead) / (2.0 * step_size)
    return minus_side, plus_side


def coordinates(first_row, cell_count, total_cells):
    indices = (first_row + jnp.arange(cell_count, dtype=jnp.int32)) % total_cells
    return -1.0 + (indices.astype(jnp.float32) + 0.5) * (2.0 / total_cells)


def advance(extended, speed_rows, first_coords, drift_matrix, drift_offset, control_bound, spacing, time_step):
    row_count = extended.shape[1] - 4
    grid_cells = extended.shape[2]
    center = lax.slice_in_dim(extended, 2, 2 + row_count, axis=1)
    gradients = [one_sided(extended, 1, spacing[0])]
    padded = jnp.pad(center, ((0, 0), (0, 0), (2, 2), (0, 0)), mode="edge")
    gradients.append(one_sided(padded, 2, spacing[1]))
    padded = jnp.pad(center, ((0, 0), (0, 0), (0, 0), (2, 2)), mode="edge")
    gradients.append(one_sided(padded, 3, spacing[2]))
    second_axis = coordinates(0, grid_cells, grid_cells)
    third_axis = coordinates(0, extended.shape[3], extended.shape[3])
    positions = (first_coords[None, :, None, None], second_axis[None, None, :, None], third_axis[None, None, None, :])
    hamiltonian = jnp.zeros_like(center)
    for d in range(3):
        drift_term = drift_offset[:, d][:, None, None, None]
        for e in range(3):
            drift_term = drift_term + drift_matrix[:, d, e][:, None, None, None] * positions[e]
        minus_side, plus_side = gradients[d]
        average = 0.5 * (minus_side + plus_side)
        reach = control_bound[:, d][:, None, None, None] * speed_rows
        hamiltonian = hamiltonian + drift_term * average - reach * jnp.abs(average) - (jnp.abs(drift_term) + reach) * 0.5 * (plus_side - minus_side)
    return jnp.minimum(center, center - time_step * hamiltonian)


def reference(value_field, speed_field, drift_matrix, drift_offset, control_bound, partner_table, dropped_dim):
    spacing = (2.0 / NX, 2.0 / N, 2.0 / N)
    time_step = min(spacing) / 15.0
    first_coords = coordinates(0, NX, NX)
    current = value_field
    for repeat in range(STEPS):
        extended = jnp.pad(current, ((0, 0), (2, 2), (0, 0), (0, 0)), mode="wrap")
        current = advance(extended, speed_field, first_coords, drift_matrix, drift_offset, control_bound, spacing, time_step)
    min_second = jnp.min(current, axis=2)
    min_third = jnp.min(current, axis=3)
    own_plane = jnp.where((dropped_dim == 1)[:, None, None], min_second, min_third)
    partner_plane = own_plane[partner_table]
    return current, jnp.maximum(own_plane, partner_plane)
```

```python
import functools

import jax
import jax.numpy as jnp
from jax import lax
from jax.experimental import pallas as pl
from jax.experimental.pallas import tpu as pltpu
from jax.sharding import PartitionSpec as P

STEPS = 2
PAD = 8
LANES = 128
MESH = pl.DeviceIdType.MESH


def pick(first, second, first_size, second_size):
    return 0.5 * jnp.where(first_size <= second_size, first, second)


def sides(cells):
    slopes = [b - a for a, b in zip(cells[:-1], cells[1:])]
    curves = [b - a for a, b in zip(slopes[:-1], slopes[1:])]
    sizes = [jnp.abs(c) for c in curves]
    picks = [
        pick(curves[k], curves[k + 1], sizes[k], sizes[k + 1]) for k in range(len(curves) - 1)
    ]
    return [
        (slopes[k + 1] + picks[k], picks[k + 1] - slopes[k + 2]) for k in range(len(picks) - 1)
    ]


def lane_shift(parts, step, ends):
    lane = lax.broadcasted_iota(jnp.int32, parts[0].shape, 1)
    rolled = [pltpu.roll(p, (LANES - step) % LANES, 1) for p in parts]
    count = len(parts)
    if step == 1:
        at_end = lane == LANES - 1
        after = [rolled[i + 1] if i + 1 < count else ends for i in range(count)]
    else:
        at_end = lane == 0
        after = [rolled[i - 1] if i > 0 else ends for i in range(count)]
    return [jnp.where(at_end, after[i], rolled[i]) for i in range(count)]


def lane_sides(parts):
    zero = jnp.zeros_like(parts[0])
    ahead = lane_shift(parts, 1, parts[-1])
    slopes = [a - v for a, v in zip(ahead, parts)]
    back_slopes = lane_shift(slopes, -1, zero)
    curves = [a - b for a, b in zip(slopes, back_slopes)]
    back_curves = lane_shift(curves, -1, zero)
    picks = [pick(b, c, jnp.abs(b), jnp.abs(c)) for b, c in zip(back_curves, curves)]
    ahead_picks = lane_shift(picks, 1, zero)
    return [(b + q, a - s) for b, q, a, s in zip(back_slopes, picks, ahead_picks, slopes)]


def kernel(
    gx_name,
    sub_name,
    value,
    speed_in,
    matrix,
    offset,
    bound,
    partner,
    dropped,
    final,
    shared,
    first,
    second,
    speed,
    result,
    minima,
    own,
    gathered,
    load_sem,
    speed_sem,
    out_sem,
    send_sem,
    recv_sem,
    plane_send,
    plane_recv,
):
    subs, rows, cells_y, cells_z = value.shape
    halves = cells_z // LANES
    count = lax.axis_size(gx_name)
    me = lax.axis_index(gx_name)
    sub_count = lax.axis_size(sub_name)
    sub_me = lax.axis_index(sub_name)
    total_rows = rows * count
    spacing = (2.0 / total_rows, 2.0 / cells_y, 2.0 / cells_z)
    time_step = min(spacing) / 15.0
    scale = [time_step / h for h in spacing]
    targets = (lax.rem(me + 1, count), lax.rem(me + count - 1, count))
    body = pl.ds(PAD, cells_y)

    loads = {}
    for s in range(subs):
        for h in range(halves):
            copy = pltpu.make_async_copy(
                value.at[s, :, :, pl.ds(h * LANES, LANES)],
                first.at[s, pl.ds(2, rows), h, body, :],
                load_sem.at[s, h],
            )
            copy.start()
            loads[s, h] = copy
        copy = pltpu.make_async_copy(speed_in.at[s], speed.at[s], speed_sem.at[s])
        copy.start()
        loads[s] = copy

    barrier = pltpu.get_barrier_semaphore()
    for target in targets:
        pl.semaphore_signal(barrier, inc=1, device_id={gx_name: target}, device_id_type=MESH)
    for k in range(1, sub_count):
        peer = lax.rem(sub_me + k, sub_count)
        pl.semaphore_signal(barrier, inc=1, device_id={sub_name: peer}, device_id_type=MESH)
    pl.semaphore_wait(barrier, 2 + sub_count - 1)

    sends = {}

    def send(step, s, side):
        for h in range(halves):
            start = rows - 2 if side == 0 else 0
            land = 0 if side == 0 else rows + 2
            if step == 0:
                source = value.at[s, pl.ds(start, 2), :, pl.ds(h * LANES, LANES)]
                sink = first.at[s, pl.ds(land, 2), h, body, :]
            else:
                source = second.at[s, pl.ds(start + 2, 2), h, body, :]
                sink = second.at[s, pl.ds(land, 2), h, body, :]
            copy = pltpu.make_async_remote_copy(
                src_ref=source,
                dst_ref=sink,
                send_sem=send_sem.at[step, s, side, h],
                recv_sem=recv_sem.at[step, s, side, h],
                device_id={gx_name: targets[side]},
                device_id_type=MESH,
            )
            copy.start()
            sends[step, s, side, h] = copy

    def receive(step, s, side):
        for h in range(halves):
            sends[step, s, side, h].wait_recv()

    for s in range(subs):
        for side in (0, 1):
            send(0, s, side)

    def pad_rows(ref, s, start, planes):
        for p in range(start, start + planes):
            for h in range(halves):
                low = ref[s, p, h, pl.ds(PAD, 1), :]
                ref[s, p, h, pl.ds(0, PAD), :] = jnp.broadcast_to(low, (PAD, LANES))
                high = ref[s, p, h, pl.ds(PAD + cells_y - 1, 1), :]
                ref[s, p, h, pl.ds(PAD + cells_y, PAD), :] = jnp.broadcast_to(high, (PAD, LANES))

    tile = (8, LANES)
    lane_index = lax.broadcasted_iota(jnp.int32, tile, 1)
    row_index = lax.broadcasted_iota(jnp.int32, tile, 0)
    z_at = [
        -1.0 + ((lane_index + h * LANES).astype(jnp.float32) + 0.5) * (2.0 / cells_z)
        for h in range(halves)
    ]

    def compute(step, s, start, planes):
        source = first if step == 0 else second
        reach = [bound[s, d] * scale[d] for d in range(3)]
        z_part = [[z * (matrix[s, d, 2] * scale[d]) for z in z_at] for d in range(3)]
        base = []
        for p in range(start, start + planes):
            x = -1.0 + ((me * rows + p).astype(jnp.float32) + 0.5) * (2.0 / total_rows)
            base.append([(offset[s, d] + matrix[s, d, 0] * x) * scale[d] for d in range(3)])

        def block(r, lows):
            at = pl.multiple_of(r * 8, 8)
            y = -1.0 + ((row_index + at).astype(jnp.float32) + 0.5) * (2.0 / cells_y)
            yz_part = []
            for d in range(3):
                y_part = y * (matrix[s, d, 1] * scale[d])
                yz_part.append([z + y_part for z in z_part[d]])
            lines = [
                [
                    source[s, p, h, pl.ds(PAD + at, 8), :]
                    for p in range(start, start + planes + 4)
                ]
                for h in range(halves)
            ]
            along_x = [sides(line) for line in lines]
            new_lows = []
            for p in range(planes):
                parts = [lines[h][p + 2] for h in range(halves)]
                along_z = lane_sides(parts)
                new = []
                for h in range(halves):
                    around = [
                        parts[h]
                        if k == 0
                        else source[s, start + p + 2, h, pl.ds(PAD + at + k, 8), :]
                        for k in (-2, -1, 0, 1, 2)
                    ]
                    along_y = sides(around)[0]
                    drift_sum = None
                    reach_sum = None
                    for d, (minus, plus_neg) in enumerate((along_x[h][p], along_y, along_z[h])):
                        drift = yz_part[d][h] + base[p][d]
                        term = jnp.abs(drift) * jnp.where(drift >= 0.0, minus, plus_neg)
                        least = reach[d] * jnp.minimum(minus, plus_neg)
                        drift_sum = term if d == 0 else drift_sum + term
                        reach_sum = least if d == 0 else reach_sum + least
                    rate = speed[s, start + p, pl.ds(at, 8), pl.ds(h * LANES, LANES)]
                    hamiltonian = drift_sum + rate * reach_sum
                    new.append(parts[h] - jnp.maximum(hamiltonian, 0.0))
                for h in range(halves):
                    if step == 0:
                        second[s, start + p + 2, h, pl.ds(PAD + at, 8), :] = new[h]
                    else:
                        result[s, start + p, pl.ds(at, 8), pl.ds(h * LANES, LANES)] = new[h]
                        new_lows.append(jnp.minimum(lows[p * halves + h], new[h]))
                if step == 1:
                    minima[p, pl.ds(at, 8), :] = functools.reduce(jnp.minimum, new)
            return tuple(new_lows)

        if step == 0:
            lax.fori_loop(0, cells_y // 8, block, ())
            pad_rows(second, s, start + 2, planes)
            return
        lows = tuple(jnp.full(tile, jnp.inf, jnp.float32) for _ in range(planes * halves))
        lows = lax.fori_loop(0, cells_y // 8, block, lows)
        copy = pltpu.make_async_copy(
            result.at[s, pl.ds(start, planes)],
            final.at[s, pl.ds(start, planes)],
            out_sem.at[s, start // 2],
        )
        copy.start()
        outs.append(copy)
        drops_second = dropped[s] == 1
        for p in range(planes):
            by_second = jnp.concatenate(
                [
                    jnp.min(lows[p * halves + h], axis=0, keepdims=True) for h in range(halves)
                ],
                axis=1,
            )
            by_third = jnp.min(minima[p].T, axis=0, keepdims=True)
            own[s, pl.ds(start + p, 1), :] = jnp.where(drops_second, by_second, by_third)

    outs = []
    last = rows - 2
    for s in range(subs):
        for h in range(halves):
            loads[s, h].wait()
        pad_rows(first, s, 2, rows)
        loads[s].wait()
        for start in range(2, last, 2):
            compute(0, s, start, 2)

    for s in range(subs):
        receive(0, s, 0)
        compute(0, s, 0, 2)
        send(1, s, 1)
        receive(0, s, 1)
        compute(0, s, last, 2)
        send(1, s, 0)
    for s in range(subs):
        for start in range(2, last, 2):
            compute(1, s, start, 2)

    plane_sends = []
    for s in range(subs):
        receive(1, s, 1)
        compute(1, s, last, 2)
        receive(1, s, 0)
        compute(1, s, 0, 2)
        gathered[sub_me * subs + s] = own[s]
        for k in range(1, sub_count):
            copy = pltpu.make_async_remote_copy(
                src_ref=own.at[s],
                dst_ref=gathered.at[sub_me * subs + s],
                send_sem=plane_send.at[s, k - 1],
                recv_sem=plane_recv.at[s, k - 1],
                device_id={sub_name: lax.rem(sub_me + k, sub_count)},
                device_id_type=MESH,
            )
            copy.start()
            plane_sends.append(copy)
    for copy in sends.values():
        copy.wait_send()
    for copy in plane_sends:
        copy.wait()
    for s in range(subs):
        shared[s] = jnp.maximum(own[s], gathered[partner[sub_me * subs + s]])
    for copy in outs:
        copy.wait()


def on_device(
    value_field, speed_field, drift_matrix, drift_offset, control_bound, partner_table, dropped_dim
):
    subs, rows, cells_y, cells_z = value_field.shape
    halves = cells_z // LANES
    sub_count = lax.axis_size("sub")
    hbm = pl.BlockSpec(memory_space=pl.ANY)
    smem = pl.BlockSpec(memory_space=pltpu.SMEM)
    vmem = pl.BlockSpec(memory_space=pltpu.VMEM)
    field = (subs, rows + 4, halves, cells_y + 2 * PAD, LANES)
    return pl.pallas_call(
        functools.partial(kernel, "gx", "sub"),
        out_shape=(
            jax.ShapeDtypeStruct(value_field.shape, jnp.float32),
            jax.ShapeDtypeStruct((subs, rows, cells_z), jnp.float32),
        ),
        in_specs=[hbm, hbm, smem, smem, smem, smem, smem],
        out_specs=(hbm, vmem),
        scratch_shapes=[
            pltpu.VMEM(field, jnp.float32),
            pltpu.VMEM(field, jnp.float32),
            pltpu.VMEM(value_field.shape, jnp.float32),
            pltpu.VMEM(value_field.shape, jnp.float32),
            pltpu.VMEM((2, cells_y, LANES), jnp.float32),
            pltpu.VMEM((subs, rows, cells_z), jnp.float32),
            pltpu.VMEM((subs * sub_count, rows, cells_z), jnp.float32),
            pltpu.SemaphoreType.DMA((subs, halves)),
            pltpu.SemaphoreType.DMA((subs,)),
            pltpu.SemaphoreType.DMA((subs, rows // 2)),
            pltpu.SemaphoreType.DMA((STEPS, subs, 2, halves)),
            pltpu.SemaphoreType.DMA((STEPS, subs, 2, halves)),
            pltpu.SemaphoreType.DMA((subs, sub_count - 1)),
            pltpu.SemaphoreType.DMA((subs, sub_count - 1)),
        ],
        compiler_params=pltpu.CompilerParams(
            collective_id=0, has_side_effects=True, vmem_limit_bytes=56 * 1024 * 1024
        ),
    )(
        value_field,
        speed_field,
        drift_matrix,
        drift_offset,
        control_bound,
        partner_table,
        dropped_dim,
    )


def solution(mesh):
    return jax.shard_map(
        on_device,
        mesh=mesh,
        in_specs=(
            P("sub", "gx", None, None),
            P("sub", "gx", None, None),
            P("sub", None, None),
            P("sub", None),
            P("sub", None),
            P(),
            P("sub"),
        ),
        out_specs=(P("sub", "gx", None, None), P("sub", "gx", None)),
        check_vma=False,
    )
```

```python
import functools

import jax
import jax.numpy as jnp
from jax import lax
from jax.experimental import pallas as pl
from jax.experimental.pallas import tpu as pltpu
from jax.sharding import PartitionSpec as P

STEPS = 2
PAD = 8
UNROLL = 4
LANES = 128
MESH = pl.DeviceIdType.MESH


def pick(first, second, first_size, second_size):
    return 0.5 * jnp.where(first_size <= second_size, first, second)


def sides(cells):
    slopes = [b - a for a, b in zip(cells[:-1], cells[1:])]
    curves = [b - a for a, b in zip(slopes[:-1], slopes[1:])]
    sizes = [jnp.abs(c) for c in curves]
    picks = [
        pick(curves[k], curves[k + 1], sizes[k], sizes[k + 1]) for k in range(len(curves) - 1)
    ]
    return [
        (slopes[k + 1] + picks[k], picks[k + 1] - slopes[k + 2]) for k in range(len(picks) - 1)
    ]


def lane_lines(parts):
    lane = lax.broadcasted_iota(jnp.int32, parts[0].shape, 1)
    count = len(parts)
    rolled = {
        step: [pltpu.roll(p, (LANES - step) % LANES, 1) for p in parts] for step in (-2, -1, 1, 2)
    }
    back_one = [
        jnp.where(lane == 0, rolled[-1][i - 1] if i else parts[0], rolled[-1][i])
        for i in range(count)
    ]
    back_two = [
        jnp.where(lane < 2, rolled[-2][i - 1] if i else back_one[0], rolled[-2][i])
        for i in range(count)
    ]
    ahead_one = [
        jnp.where(
            lane == LANES - 1, rolled[1][i + 1] if i + 1 < count else parts[i], rolled[1][i]
        )
        for i in range(count)
    ]
    ahead_two = [
        jnp.where(
            lane >= LANES - 2, rolled[2][i + 1] if i + 1 < count else ahead_one[i], rolled[2][i]
        )
        for i in range(count)
    ]
    return list(zip(back_two, back_one, parts, ahead_one, ahead_two))


def kernel(
    gx_name,
    sub_name,
    value,
    speed_in,
    matrix,
    offset,
    bound,
    partner,
    dropped,
    final,
    shared,
    first,
    second,
    speed,
    result,
    minima,
    own,
    gathered,
    load_sem,
    speed_sem,
    out_sem,
    send_sem,
    recv_sem,
    plane_send,
    plane_recv,
):
    subs, rows, cells_y, cells_z = value.shape
    halves = cells_z // LANES
    count = lax.axis_size(gx_name)
    me = lax.axis_index(gx_name)
    sub_count = lax.axis_size(sub_name)
    sub_me = lax.axis_index(sub_name)
    total_rows = rows * count
    spacing = (2.0 / total_rows, 2.0 / cells_y, 2.0 / cells_z)
    time_step = min(spacing) / 15.0
    scale = [time_step / h for h in spacing]
    targets = (lax.rem(me + 1, count), lax.rem(me + count - 1, count))
    body = pl.ds(PAD, cells_y)

    loads = {}
    for s in range(subs):
        for h in range(halves):
            copy = pltpu.make_async_copy(
                value.at[s, :, :, pl.ds(h * LANES, LANES)],
                first.at[s, pl.ds(2, rows), h, body, :],
                load_sem.at[s, h],
            )
            copy.start()
            loads[s, h] = copy
        copy = pltpu.make_async_copy(speed_in.at[s], speed.at[s], speed_sem.at[s])
        copy.start()
        loads[s] = copy

    barrier = pltpu.get_barrier_semaphore()
    for target in targets:
        pl.semaphore_signal(barrier, inc=1, device_id={gx_name: target}, device_id_type=MESH)
    for k in range(1, sub_count):
        peer = lax.rem(sub_me + k, sub_count)
        pl.semaphore_signal(barrier, inc=1, device_id={sub_name: peer}, device_id_type=MESH)
    pl.semaphore_wait(barrier, 2 + sub_count - 1)

    sends = {}

    def send(step, s, side):
        for h in range(halves):
            start = rows - 2 if side == 0 else 0
            land = 0 if side == 0 else rows + 2
            if step == 0:
                source = value.at[s, pl.ds(start, 2), :, pl.ds(h * LANES, LANES)]
                sink = first.at[s, pl.ds(land, 2), h, body, :]
            else:
                source = second.at[s, pl.ds(start + 2, 2), h, body, :]
                sink = second.at[s, pl.ds(land, 2), h, body, :]
            copy = pltpu.make_async_remote_copy(
                src_ref=source,
                dst_ref=sink,
                send_sem=send_sem.at[step, s, side, h],
                recv_sem=recv_sem.at[step, s, side, h],
                device_id={gx_name: targets[side]},
                device_id_type=MESH,
            )
            copy.start()
            sends[step, s, side, h] = copy

    def receive(step, s, side):
        for h in range(halves):
            sends[step, s, side, h].wait_recv()

    for s in range(subs):
        for side in (0, 1):
            send(0, s, side)

    def pad_rows(ref, s, start, planes):
        for p in range(start, start + planes):
            for h in range(halves):
                low = ref[s, p, h, pl.ds(PAD, 1), :]
                ref[s, p, h, pl.ds(0, PAD), :] = jnp.broadcast_to(low, (PAD, LANES))
                high = ref[s, p, h, pl.ds(PAD + cells_y - 1, 1), :]
                ref[s, p, h, pl.ds(PAD + cells_y, PAD), :] = jnp.broadcast_to(high, (PAD, LANES))

    tile = (8, LANES)
    lane_index = lax.broadcasted_iota(jnp.int32, tile, 1)
    row_index = lax.broadcasted_iota(jnp.int32, tile, 0)
    z_at = [
        -1.0 + ((lane_index + h * LANES).astype(jnp.float32) + 0.5) * (2.0 / cells_z)
        for h in range(halves)
    ]

    def compute(step, s, start, planes):
        source = first if step == 0 else second
        reach = [bound[s, d] * scale[d] for d in range(3)]
        z_part = [[z * (matrix[s, d, 2] * scale[d]) for z in z_at] for d in range(3)]
        base = []
        for p in range(start, start + planes):
            x = -1.0 + ((me * rows + p).astype(jnp.float32) + 0.5) * (2.0 / total_rows)
            base.append([(offset[s, d] + matrix[s, d, 0] * x) * scale[d] for d in range(3)])

        def block(r, lows):
            at = pl.multiple_of(r * 8, 8)
            y = -1.0 + ((row_index + at).astype(jnp.float32) + 0.5) * (2.0 / cells_y)
            yz_part = []
            for d in range(3):
                y_part = y * (matrix[s, d, 1] * scale[d])
                yz_part.append([z + y_part for z in z_part[d]])
            lines = [
                [
                    source[s, p, h, pl.ds(PAD + at, 8), :]
                    for p in range(start, start + planes + 4)
                ]
                for h in range(halves)
            ]
            along_x = [sides(line) for line in lines]
            new_lows = []
            for p in range(planes):
                parts = [lines[h][p + 2] for h in range(halves)]
                along_z = [sides(line)[0] for line in lane_lines(parts)]
                new = []
                for h in range(halves):
                    around = [
                        parts[h]
                        if k == 0
                        else source[s, start + p + 2, h, pl.ds(PAD + at + k, 8), :]
                        for k in (-2, -1, 0, 1, 2)
                    ]
                    along_y = sides(around)[0]
                    drift_sum = None
                    reach_sum = None
                    for d, (minus, plus_neg) in enumerate((along_x[h][p], along_y, along_z[h])):
                        drift = yz_part[d][h] + base[p][d]
                        term = jnp.abs(drift) * jnp.where(drift >= 0.0, minus, plus_neg)
                        least = reach[d] * jnp.minimum(minus, plus_neg)
                        drift_sum = term if d == 0 else drift_sum + term
                        reach_sum = least if d == 0 else reach_sum + least
                    rate = speed[s, start + p, pl.ds(at, 8), pl.ds(h * LANES, LANES)]
                    hamiltonian = drift_sum + rate * reach_sum
                    new.append(parts[h] - jnp.maximum(hamiltonian, 0.0))
                for h in range(halves):
                    if step == 0:
                        second[s, start + p + 2, h, pl.ds(PAD + at, 8), :] = new[h]
                    else:
                        result[s, start + p, pl.ds(at, 8), pl.ds(h * LANES, LANES)] = new[h]
                        new_lows.append(jnp.minimum(lows[p * halves + h], new[h]))
                if step == 1:
                    minima[p, pl.ds(at, 8), :] = functools.reduce(jnp.minimum, new)
            return tuple(new_lows)

        if step == 0:
            lax.fori_loop(0, cells_y // 8, block, (), unroll=UNROLL)
            pad_rows(second, s, start + 2, planes)
            return
        lows = tuple(jnp.full(tile, jnp.inf, jnp.float32) for _ in range(planes * halves))
        lows = lax.fori_loop(0, cells_y // 8, block, lows, unroll=UNROLL)
        copy = pltpu.make_async_copy(
            result.at[s, pl.ds(start, planes)],
            final.at[s, pl.ds(start, planes)],
            out_sem.at[s, start // 2],
        )
        copy.start()
        outs.append(copy)
        drops_second = dropped[s] == 1
        for p in range(planes):
            by_second = jnp.concatenate(
                [
                    jnp.min(lows[p * halves + h], axis=0, keepdims=True) for h in range(halves)
                ],
                axis=1,
            )
            by_third = jnp.min(minima[p].T, axis=0, keepdims=True)
            own[s, pl.ds(start + p, 1), :] = jnp.where(drops_second, by_second, by_third)

    outs = []
    last = rows - 2
    for s in range(subs):
        for h in range(halves):
            loads[s, h].wait()
        pad_rows(first, s, 2, rows)
        loads[s].wait()
        for start in range(2, last, 2):
            compute(0, s, start, 2)

    for s in range(subs):
        receive(0, s, 0)
        compute(0, s, 0, 2)
        send(1, s, 1)
        receive(0, s, 1)
        compute(0, s, last, 2)
        send(1, s, 0)
    for s in range(subs):
        for start in range(2, last, 2):
            compute(1, s, start, 2)

    plane_sends = []
    for s in range(subs):
        receive(1, s, 1)
        compute(1, s, last, 2)
        receive(1, s, 0)
        compute(1, s, 0, 2)
        gathered[sub_me * subs + s] = own[s]
        for k in range(1, sub_count):
            copy = pltpu.make_async_remote_copy(
                src_ref=own.at[s],
                dst_ref=gathered.at[sub_me * subs + s],
                send_sem=plane_send.at[s, k - 1],
                recv_sem=plane_recv.at[s, k - 1],
                device_id={sub_name: lax.rem(sub_me + k, sub_count)},
                device_id_type=MESH,
            )
            copy.start()
            plane_sends.append(copy)
    for copy in sends.values():
        copy.wait_send()
    for copy in plane_sends:
        copy.wait()
    for s in range(subs):
        shared[s] = jnp.maximum(own[s], gathered[partner[sub_me * subs + s]])
    for copy in outs:
        copy.wait()


def on_device(
    value_field, speed_field, drift_matrix, drift_offset, control_bound, partner_table, dropped_dim
):
    subs, rows, cells_y, cells_z = value_field.shape
    halves = cells_z // LANES
    sub_count = lax.axis_size("sub")
    hbm = pl.BlockSpec(memory_space=pl.ANY)
    smem = pl.BlockSpec(memory_space=pltpu.SMEM)
    vmem = pl.BlockSpec(memory_space=pltpu.VMEM)
    field = (subs, rows + 4, halves, cells_y + 2 * PAD, LANES)
    return pl.pallas_call(
        functools.partial(kernel, "gx", "sub"),
        out_shape=(
            jax.ShapeDtypeStruct(value_field.shape, jnp.float32),
            jax.ShapeDtypeStruct((subs, rows, cells_z), jnp.float32),
        ),
        in_specs=[hbm, hbm, smem, smem, smem, smem, smem],
        out_specs=(hbm, vmem),
        scratch_shapes=[
            pltpu.VMEM(field, jnp.float32),
            pltpu.VMEM(field, jnp.float32),
            pltpu.VMEM(value_field.shape, jnp.float32),
            pltpu.VMEM(value_field.shape, jnp.float32),
            pltpu.VMEM((2, cells_y, LANES), jnp.float32),
            pltpu.VMEM((subs, rows, cells_z), jnp.float32),
            pltpu.VMEM((subs * sub_count, rows, cells_z), jnp.float32),
            pltpu.SemaphoreType.DMA((subs, halves)),
            pltpu.SemaphoreType.DMA((subs,)),
            pltpu.SemaphoreType.DMA((subs, rows // 2)),
            pltpu.SemaphoreType.DMA((STEPS, subs, 2, halves)),
            pltpu.SemaphoreType.DMA((STEPS, subs, 2, halves)),
            pltpu.SemaphoreType.DMA((subs, sub_count - 1)),
            pltpu.SemaphoreType.DMA((subs, sub_count - 1)),
        ],
        compiler_params=pltpu.CompilerParams(
            collective_id=0, has_side_effects=True, vmem_limit_bytes=56 * 1024 * 1024
        ),
    )(
        value_field,
        speed_field,
        drift_matrix,
        drift_offset,
        control_bound,
        partner_table,
        dropped_dim,
    )


def solution(mesh):
    return jax.shard_map(
        on_device,
        mesh=mesh,
        in_specs=(
            P("sub", "gx", None, None),
            P("sub", "gx", None, None),
            P("sub", None, None),
            P("sub", None),
            P("sub", None),
            P(),
            P("sub"),
        ),
        out_specs=(P("sub", "gx", None, None), P("sub", "gx", None)),
        check_vma=False,
    )
```

```python
import functools

import jax
import jax.numpy as jnp
from jax import lax
from jax.experimental import pallas as pl
from jax.experimental.pallas import tpu as pltpu
from jax.sharding import PartitionSpec as P

STEPS = 2
PAD = 8
UNROLL = 4
LANES = 128
MESH = pl.DeviceIdType.MESH


def pick(first, second, first_size, second_size):
    return 0.5 * jnp.where(first_size <= second_size, first, second)


def sides(cells):
    slopes = [b - a for a, b in zip(cells[:-1], cells[1:])]
    curves = [b - a for a, b in zip(slopes[:-1], slopes[1:])]
    sizes = [jnp.abs(c) for c in curves]
    picks = [
        pick(curves[k], curves[k + 1], sizes[k], sizes[k + 1]) for k in range(len(curves) - 1)
    ]
    return [
        (slopes[k + 1] + picks[k], picks[k + 1] - slopes[k + 2]) for k in range(len(picks) - 1)
    ]


def lane_lines(parts):
    lane = lax.broadcasted_iota(jnp.int32, parts[0].shape, 1)
    count = len(parts)
    rolled = {
        step: [pltpu.roll(p, (LANES - step) % LANES, 1) for p in parts] for step in (-2, -1, 1, 2)
    }
    back_one = [
        jnp.where(lane == 0, rolled[-1][i - 1] if i else parts[0], rolled[-1][i])
        for i in range(count)
    ]
    back_two = [
        jnp.where(lane < 2, rolled[-2][i - 1] if i else back_one[0], rolled[-2][i])
        for i in range(count)
    ]
    ahead_one = [
        jnp.where(
            lane == LANES - 1, rolled[1][i + 1] if i + 1 < count else parts[i], rolled[1][i]
        )
        for i in range(count)
    ]
    ahead_two = [
        jnp.where(
            lane >= LANES - 2, rolled[2][i + 1] if i + 1 < count else ahead_one[i], rolled[2][i]
        )
        for i in range(count)
    ]
    return list(zip(back_two, back_one, parts, ahead_one, ahead_two))


def kernel(
    gx_name,
    sub_name,
    value,
    speed_in,
    matrix,
    offset,
    bound,
    partner,
    dropped,
    final,
    shared,
    first,
    second,
    speed,
    result,
    minima,
    own,
    gathered,
    load_sem,
    speed_sem,
    out_sem,
    send_sem,
    recv_sem,
    plane_send,
    plane_recv,
):
    subs, rows, cells_y, cells_z = value.shape
    halves = cells_z // LANES
    count = lax.axis_size(gx_name)
    me = lax.axis_index(gx_name)
    sub_count = lax.axis_size(sub_name)
    sub_me = lax.axis_index(sub_name)
    total_rows = rows * count
    spacing = (2.0 / total_rows, 2.0 / cells_y, 2.0 / cells_z)
    time_step = min(spacing) / 15.0
    scale = [time_step / h for h in spacing]
    targets = (lax.rem(me + 1, count), lax.rem(me + count - 1, count))
    body = pl.ds(PAD, cells_y)

    loads = {}
    for s in range(subs):
        for h in range(halves):
            copy = pltpu.make_async_copy(
                value.at[s, :, :, pl.ds(h * LANES, LANES)],
                first.at[s, pl.ds(2, rows), h, body, :],
                load_sem.at[s, h],
            )
            copy.start()
            loads[s, h] = copy
        copy = pltpu.make_async_copy(speed_in.at[s], speed.at[s], speed_sem.at[s])
        copy.start()
        loads[s] = copy

    barrier = pltpu.get_barrier_semaphore()
    for target in targets:
        pl.semaphore_signal(barrier, inc=1, device_id={gx_name: target}, device_id_type=MESH)
    for k in range(1, sub_count):
        peer = lax.rem(sub_me + k, sub_count)
        pl.semaphore_signal(barrier, inc=1, device_id={sub_name: peer}, device_id_type=MESH)
    pl.semaphore_wait(barrier, 2 + sub_count - 1)

    sends = {}

    def send(step, s, side):
        start = rows - 2 if side == 0 else 0
        land = 0 if side == 0 else rows + 2
        for h in range(halves if step == 0 else 1):
            if step == 0:
                source = value.at[s, pl.ds(start, 2), :, pl.ds(h * LANES, LANES)]
                sink = first.at[s, pl.ds(land, 2), h, body, :]
            else:
                source = second.at[s, pl.ds(start + 2, 2), :, body, :]
                sink = second.at[s, pl.ds(land, 2), :, body, :]
            copy = pltpu.make_async_remote_copy(
                src_ref=source,
                dst_ref=sink,
                send_sem=send_sem.at[step, s, side, h],
                recv_sem=recv_sem.at[step, s, side, h],
                device_id={gx_name: targets[side]},
                device_id_type=MESH,
            )
            copy.start()
            sends[step, s, side, h] = copy

    def receive(step, s, side):
        for h in range(halves if step == 0 else 1):
            sends[step, s, side, h].wait_recv()

    for s in range(subs):
        for side in (0, 1):
            send(0, s, side)

    def pad_rows(ref, s, start, planes):
        for p in range(start, start + planes):
            for h in range(halves):
                low = ref[s, p, h, pl.ds(PAD, 1), :]
                ref[s, p, h, pl.ds(0, PAD), :] = jnp.broadcast_to(low, (PAD, LANES))
                high = ref[s, p, h, pl.ds(PAD + cells_y - 1, 1), :]
                ref[s, p, h, pl.ds(PAD + cells_y, PAD), :] = jnp.broadcast_to(high, (PAD, LANES))

    tile = (8, LANES)
    lane_index = lax.broadcasted_iota(jnp.int32, tile, 1)
    row_index = lax.broadcasted_iota(jnp.int32, tile, 0)
    z_at = [
        -1.0 + ((lane_index + h * LANES).astype(jnp.float32) + 0.5) * (2.0 / cells_z)
        for h in range(halves)
    ]

    def compute(step, s, start, planes):
        source = first if step == 0 else second
        reach = [bound[s, d] * scale[d] for d in range(3)]
        z_part = [[z * (matrix[s, d, 2] * scale[d]) for z in z_at] for d in range(3)]
        base = []
        for p in range(start, start + planes):
            x = -1.0 + ((me * rows + p).astype(jnp.float32) + 0.5) * (2.0 / total_rows)
            base.append([(offset[s, d] + matrix[s, d, 0] * x) * scale[d] for d in range(3)])

        def block(r, lows):
            at = pl.multiple_of(r * 8, 8)
            y = -1.0 + ((row_index + at).astype(jnp.float32) + 0.5) * (2.0 / cells_y)
            yz_part = []
            for d in range(3):
                y_part = y * (matrix[s, d, 1] * scale[d])
                yz_part.append([z + y_part for z in z_part[d]])
            lines = [
                [
                    source[s, p, h, pl.ds(PAD + at, 8), :]
                    for p in range(start, start + planes + 4)
                ]
                for h in range(halves)
            ]
            along_x = [sides(line) for line in lines]
            new_lows = []
            for p in range(planes):
                parts = [lines[h][p + 2] for h in range(halves)]
                along_z = [sides(line)[0] for line in lane_lines(parts)]
                new = []
                for h in range(halves):
                    around = [
                        parts[h]
                        if k == 0
                        else source[s, start + p + 2, h, pl.ds(PAD + at + k, 8), :]
                        for k in (-2, -1, 0, 1, 2)
                    ]
                    along_y = sides(around)[0]
                    drift_sum = None
                    reach_sum = None
                    for d, (minus, plus_neg) in enumerate((along_x[h][p], along_y, along_z[h])):
                        drift = yz_part[d][h] + base[p][d]
                        term = jnp.abs(drift) * jnp.where(drift >= 0.0, minus, plus_neg)
                        least = reach[d] * jnp.minimum(minus, plus_neg)
                        drift_sum = term if d == 0 else drift_sum + term
                        reach_sum = least if d == 0 else reach_sum + least
                    rate = speed[s, start + p, pl.ds(at, 8), pl.ds(h * LANES, LANES)]
                    hamiltonian = drift_sum + rate * reach_sum
                    new.append(parts[h] - jnp.maximum(hamiltonian, 0.0))
                for h in range(halves):
                    if step == 0:
                        second[s, start + p + 2, h, pl.ds(PAD + at, 8), :] = new[h]
                    else:
                        result[s, start + p, pl.ds(at, 8), pl.ds(h * LANES, LANES)] = new[h]
                        new_lows.append(jnp.minimum(lows[p * halves + h], new[h]))
                if step == 1:
                    minima[p, pl.ds(at, 8), :] = functools.reduce(jnp.minimum, new)
            return tuple(new_lows)

        if step == 0:
            lax.fori_loop(0, cells_y // 8, block, (), unroll=UNROLL)
            pad_rows(second, s, start + 2, planes)
            return
        lows = tuple(jnp.full(tile, jnp.inf, jnp.float32) for _ in range(planes * halves))
        lows = lax.fori_loop(0, cells_y // 8, block, lows, unroll=UNROLL)
        copy = pltpu.make_async_copy(
            result.at[s, pl.ds(start, planes)],
            final.at[s, pl.ds(start, planes)],
            out_sem.at[s, start // 2],
        )
        copy.start()
        outs.append(copy)
        drops_second = dropped[s] == 1
        for p in range(planes):
            by_second = jnp.concatenate(
                [
                    jnp.min(lows[p * halves + h], axis=0, keepdims=True) for h in range(halves)
                ],
                axis=1,
            )
            by_third = jnp.min(minima[p].T, axis=0, keepdims=True)
            own[s, pl.ds(start + p, 1), :] = jnp.where(drops_second, by_second, by_third)

    outs = []
    last = rows - 2
    for s in range(subs):
        for h in range(halves):
            loads[s, h].wait()
        pad_rows(first, s, 2, rows)
        loads[s].wait()
        for start in range(2, last, 2):
            compute(0, s, start, 2)

    for s in range(subs):
        receive(0, s, 0)
        compute(0, s, 0, 2)
        receive(0, s, 1)
        compute(0, s, last, 2)
        send(1, s, 0)
        send(1, s, 1)
    for s in range(subs):
        for start in range(2, last, 2):
            compute(1, s, start, 2)

    plane_sends = []
    for s in range(subs):
        receive(1, s, 0)
        compute(1, s, 0, 2)
        receive(1, s, 1)
        compute(1, s, last, 2)
        gathered[sub_me * subs + s] = own[s]
        for k in range(1, sub_count):
            copy = pltpu.make_async_remote_copy(
                src_ref=own.at[s],
                dst_ref=gathered.at[sub_me * subs + s],
                send_sem=plane_send.at[s, k - 1],
                recv_sem=plane_recv.at[s, k - 1],
                device_id={sub_name: lax.rem(sub_me + k, sub_count)},
                device_id_type=MESH,
            )
            copy.start()
            plane_sends.append(copy)
    for copy in sends.values():
        copy.wait_send()
    for copy in plane_sends:
        copy.wait()
    for s in range(subs):
        shared[s] = jnp.maximum(own[s], gathered[partner[sub_me * subs + s]])
    for copy in outs:
        copy.wait()


def on_device(
    value_field, speed_field, drift_matrix, drift_offset, control_bound, partner_table, dropped_dim
):
    subs, rows, cells_y, cells_z = value_field.shape
    halves = cells_z // LANES
    sub_count = lax.axis_size("sub")
    hbm = pl.BlockSpec(memory_space=pl.ANY)
    smem = pl.BlockSpec(memory_space=pltpu.SMEM)
    vmem = pl.BlockSpec(memory_space=pltpu.VMEM)
    field = (subs, rows + 4, halves, cells_y + 2 * PAD, LANES)
    return pl.pallas_call(
        functools.partial(kernel, "gx", "sub"),
        out_shape=(
            jax.ShapeDtypeStruct(value_field.shape, jnp.float32),
            jax.ShapeDtypeStruct((subs, rows, cells_z), jnp.float32),
        ),
        in_specs=[hbm, hbm, smem, smem, smem, smem, smem],
        out_specs=(hbm, vmem),
        scratch_shapes=[
            pltpu.VMEM(field, jnp.float32),
            pltpu.VMEM(field, jnp.float32),
            pltpu.VMEM(value_field.shape, jnp.float32),
            pltpu.VMEM(value_field.shape, jnp.float32),
            pltpu.VMEM((2, cells_y, LANES), jnp.float32),
            pltpu.VMEM((subs, rows, cells_z), jnp.float32),
            pltpu.VMEM((subs * sub_count, rows, cells_z), jnp.float32),
            pltpu.SemaphoreType.DMA((subs, halves)),
            pltpu.SemaphoreType.DMA((subs,)),
            pltpu.SemaphoreType.DMA((subs, rows // 2)),
            pltpu.SemaphoreType.DMA((STEPS, subs, 2, halves)),
            pltpu.SemaphoreType.DMA((STEPS, subs, 2, halves)),
            pltpu.SemaphoreType.DMA((subs, sub_count - 1)),
            pltpu.SemaphoreType.DMA((subs, sub_count - 1)),
        ],
        compiler_params=pltpu.CompilerParams(
            collective_id=0, has_side_effects=True, vmem_limit_bytes=56 * 1024 * 1024
        ),
    )(
        value_field,
        speed_field,
        drift_matrix,
        drift_offset,
        control_bound,
        partner_table,
        dropped_dim,
    )


def solution(mesh):
    return jax.shard_map(
        on_device,
        mesh=mesh,
        in_specs=(
            P("sub", "gx", None, None),
            P("sub", "gx", None, None),
            P("sub", None, None),
            P("sub", None),
            P("sub", None),
            P(),
            P("sub"),
        ),
        out_specs=(P("sub", "gx", None, None), P("sub", "gx", None)),
        check_vma=False,
    )
```
